32 devices in a mesh: groups: 2 (over x), ep: 8 (over z, y), node: 2 (over core).
Axes of the slice: x: 2, y: 2, z: 4, core: 2. Of those that a mesh axis runs over, the one named last changes fastest.
Arguments:
- tokens: bfloat16 [1024, 7168], P(('groups', 'ep', 'node')), parts along dimension 0, may hold values from -6 to 6
- expert_ids: int32 [1024, 8], P(('groups', 'ep', 'node')), parts along dimension 0, may hold values from 0 to 15, all different within a row; in each aligned block of 32 rows (0 to 31, 32 to 63, ...) at most 32 rows name the same one
- gate_weights: float32 [1024, 8], P(('groups', 'ep', 'node')), parts along dimension 0, may hold values from 0.05 to 0.5
- gate_up_weight: bfloat16 [16, 7168, 512], P(('ep', 'node')), may hold values from -0.0625 to 0.0625
- down_weight: bfloat16 [16, 256, 7168], P(('ep', 'node')), may hold values from -0.375 to 0.375
Outputs:
- moe_out: bfloat16 [1024, 7168], P(('groups', 'ep', 'node')), parts along dimension 0
The draws below stay inside these ranges and needn't reach their ends.
There are 2 independent parts, one for each index of `groups`. The reference program is written for one: setup_inputs(seed, part) draws one part's arguments, and reference() takes and returns one part's arrays. A program takes and returns all parts, laid end to end along the dimension named above; an argument that names none is the same for every part. Nothing has to cross between parts.
Inputs may be any that keep to these rules, and one draw needn't show every extreme that they name: `expert_ids`: each token names 8 different experts; among the 32 tokens of one device no expert is named by more than 32 of them, a bound that some block reaches.
All inputs are finite; a program needn't handle non-finite values.
Results may differ from the reference program's by a relative error of at most 0.0058.
Values may be sent and summed in bfloat16 or wider, within the bound.
A program may use at most 128 MiB of HBM per device.

```python
import math
import jax
import jax.numpy as jnp
import numpy as np
from jax import lax

D = 7168
TOP = 8
EXP_HID = 256
TOK_DEV = 32
EXPERTS = 16
CAP = 32
TOKENS = 512
N_EP = 8
N_NODE = 2


def level_of(rng, dims, split, smallest, high):
    level = 1.0
    for axis_at, blocks in split:
        heights = jax.random.uniform(jax.random.fold_in(jax.random.fold_in(rng, 6), axis_at), (blocks,), jnp.float32, smallest / len(split), high / len(split))
        level = level * jnp.repeat(jnp.exp(heights), dims[axis_at] // blocks).reshape((-1,) + (1,) * (len(dims) - 1 - axis_at))
    return level


def assign_block(rng, own, number, rows, count, top, most, slope):
    sequence = jax.random.permutation(rng, count)
    heavy_load, common = load_shares(count, rows * top, most, slope, True), load_shares(count, rows * top, most, slope, False)
    places = jnp.arange(count)

    def named(sizes, turn):
        used = int((sizes > 0).sum())
        fixed = max(1, used // 4)
        shifted = fixed + (places - fixed + turn * (used - fixed)) % max(1, count - fixed)
        return jnp.zeros((count,), jnp.int32).at[sequence[jnp.where(places < fixed, places, shifted)]].set(jnp.asarray(sizes, jnp.int32))

    sizes = jnp.where(number % 4 == 0, named(heavy_load, number // 4), named(common, number - number // 4 - 1))
    mixed = jax.random.permutation(jax.random.fold_in(own, 3), count)
    source_of, taker = mixed[0:count // 2 * 2:2], mixed[1:count // 2 * 2:2]
    room = jnp.minimum(sizes[source_of] - 1, most - sizes[taker]) // 2
    room = jnp.where((source_of == sequence[0]) | (taker == sequence[0]) | (sizes[taker] == 0), 0, jnp.maximum(room, 0))
    shifted = jax.random.randint(jax.random.fold_in(own, 4), (count // 2,), 0, 1 << 20) % (room + 1)
    sizes = sizes.at[source_of].add(-shifted).at[taker].add(shifted)
    members = jnp.searchsorted(jnp.cumsum(sizes), jnp.arange(rows * top), side="right").astype(jnp.int32)
    table = members.reshape(top, rows).T
    table = table[jax.random.permutation(jax.random.fold_in(own, 1), rows)]
    turn = jax.random.randint(jax.random.fold_in(own, 2), (rows, 1), 0, top)
    return jnp.take_along_axis(table, (jnp.arange(top)[None, :] + turn) % top, axis=1)


def load_shares(amount, total, reach, skew, full):
    weights = [(1 << 20) // math.isqrt(grade ** skew) + 1 for grade in range(1, amount + 1)]
    largest = reach if full else min(reach, max(-(-total // amount), total * weights[0] // sum(weights)))
    least = 1 if total - largest >= amount - 1 else 0
    given, rest = [largest] + [least] * (amount - 1), total - largest - least * (amount - 1)
    while rest > 0:
        free = [i for i in range(1, amount) if given[i] < largest] or [i for i in range(1, amount) if given[i] < reach]
        pool, left = sum([weights[i] for i in free]), rest
        for i in free:
            extra = min(reach - given[i], max(1, left * weights[i] // pool), rest)
            given[i] = given[i] + extra
            rest = rest - extra
    return np.array(given)


def normal_values(key, extent, spread, reach, cuts=(), held_as=jnp.bfloat16):
    drawn = spread * jax.random.normal(key, extent, jnp.float32)
    if cuts:
        drawn = drawn * level_of(key, extent, cuts, -0.22, 0.18)
    return jnp.clip(drawn, -reach, reach).astype(held_as)


def setup_inputs(seed: int = 0, part: int = 0) -> dict:
    splits = jax.random.split(jax.random.key(seed), 6)
    part_keys = jax.random.split(jax.random.fold_in(splits[5], part), 6)
    tokens = normal_values(part_keys[0], (TOKENS, D), 1.0, 6.0, ((0, 16),))
    expert_ids_keys = jax.random.split(jax.random.fold_in(part_keys[1], 1), TOKENS // TOK_DEV)
    expert_ids_turns = jax.random.permutation(jax.random.fold_in(part_keys[1], 3), TOKENS // TOK_DEV)
    expert_ids = jax.vmap(lambda own, number: assign_block(jax.random.fold_in(part_keys[1], 2), own, number, TOK_DEV, EXPERTS, TOP, CAP, 2))(expert_ids_keys, expert_ids_turns).reshape((TOKENS, TOP))
    gate_weights = jnp.clip(jnp.exp(math.log(0.5) - 2.3025851 * jax.random.uniform(part_keys[2], (TOKENS, TOP), jnp.float32) ** level_of(part_keys[2], (TOKENS, TOP), ((0, 16),), -0.2, 0.2)), 0.05, 0.5)
    gate_up_weight = normal_values(splits[3], (EXPERTS, D, 2 * EXP_HID), D ** -0.5, 0.0625, ((0, 16),))
    down_weight = normal_values(splits[4], (EXPERTS, EXP_HID, D), EXP_HID ** -0.5, 0.375, ((0, 16),))
    return {"tokens": tokens, "expert_ids": expert_ids, "gate_weights": gate_weights, "gate_up_weight": gate_up_weight, "down_weight": down_weight}


def reference(tokens, expert_ids, gate_weights, gate_up_weight, down_weight):
    slot_total = N_EP * N_NODE * CAP
    token_index = jnp.arange(TOKENS, dtype=jnp.int32)

    def per_expert(running, expert):
        chosen = expert_ids == expert
        routed = jnp.any(chosen, axis=1)
        picked = jnp.sum(jnp.where(chosen, gate_weights, jnp.zeros_like(gate_weights)), axis=1)
        position = jnp.cumsum(routed.astype(jnp.int32)) - 1
        where_to = jnp.where(routed, position, slot_total).astype(jnp.int32)
        row_index = jnp.zeros((slot_total,), jnp.int32).at[where_to].set(token_index, mode="drop")
        filled = jnp.zeros((slot_total,), jnp.float32).at[where_to].set(jnp.ones((TOKENS,), jnp.float32), mode="drop")
        gathered = tokens[row_index]
        gate_up = jnp.dot(gathered, gate_up_weight[expert], preferred_element_type=jnp.float32)
        hidden = (jax.nn.silu(gate_up[:, :EXP_HID]) * gate_up[:, EXP_HID:]).astype(jnp.bfloat16)
        result = jnp.dot(hidden, down_weight[expert], preferred_element_type=jnp.float32).astype(jnp.bfloat16)
        weight_row = filled * picked[row_index]
        running = running.at[row_index].add(weight_row[:, None] * result.astype(jnp.float32))
        return running, None

    start = jnp.zeros((TOKENS, D), jnp.float32)
    summed, unused = lax.scan(per_expert, start, jnp.arange(EXPERTS, dtype=jnp.int32))
    return summed.astype(jnp.bfloat16)
```

```python
import jax
import jax.numpy as jnp
from jax import lax
from jax.sharding import PartitionSpec as P

AXES = ("ep", "node")


def on_device(tokens, expert_ids, gate_weights, gate_up_weight, down_weight):
    local_count, inner_width = down_weight.shape[0], down_weight.shape[1]
    device = lax.axis_index("ep") * lax.axis_size("node") + lax.axis_index("node")
    all_tokens = lax.all_gather(tokens, AXES, axis=0, tiled=True)
    all_ids = lax.all_gather(expert_ids, AXES, axis=0, tiled=True)
    all_weights = lax.all_gather(gate_weights, AXES, axis=0, tiled=True)
    total = 0.0
    for local in range(local_count):
        expert = device * local_count + local
        share = jnp.sum(jnp.where(all_ids == expert, all_weights, 0.0), axis=1)
        gate_up = jnp.dot(all_tokens, gate_up_weight[local], preferred_element_type=jnp.float32)
        hidden = (jax.nn.silu(gate_up[:, :inner_width]) * gate_up[:, inner_width:]).astype(
            jnp.bfloat16
        )
        product = jnp.dot(hidden, down_weight[local], preferred_element_type=jnp.float32)
        total = total + share[:, None] * product
    return lax.psum_scatter(total.astype(jnp.bfloat16), AXES, scatter_dimension=0, tiled=True)


def solution(mesh):
    placed = (
        P(("groups", "ep", "node"), None),
        P(("groups", "ep", "node"), None),
        P(("groups", "ep", "node"), None),
        P(("ep", "node"), None, None),
        P(("ep", "node"), None, None),
    )
    return jax.shard_map(
        on_device,
        mesh=mesh,
        in_specs=placed,
        out_specs=P(("groups", "ep", "node"), None),
        check_vma=False,
    )
```

```python
import functools

import jax
import jax.numpy as jnp
from jax import lax
from jax.experimental import pallas as pl
from jax.experimental.pallas import tpu as pltpu
from jax.sharding import PartitionSpec as P

AXES = ("ep", "node")
PAIR = 2
PIECES = 2
LANES = 128
VMEM_BYTES = 60 * 1024 * 1024
MESH = pl.DeviceIdType.MESH


def spread_out(tokens, expert_ids, gate_weights, gate_up_weight, down_weight):
    local_count, inner_width = down_weight.shape[0], down_weight.shape[1]
    device = lax.axis_index("ep") * lax.axis_size("node") + lax.axis_index("node")
    all_tokens = lax.all_gather(tokens, AXES, axis=0, tiled=True)
    all_ids = lax.all_gather(expert_ids, AXES, axis=0, tiled=True)
    all_weights = lax.all_gather(gate_weights, AXES, axis=0, tiled=True)
    total = 0.0
    for local in range(local_count):
        expert = device * local_count + local
        share = jnp.sum(jnp.where(all_ids == expert, all_weights, 0.0), axis=1)
        gate_up = jnp.dot(all_tokens, gate_up_weight[local], preferred_element_type=jnp.float32)
        hidden = (jax.nn.silu(gate_up[:, :inner_width]) * gate_up[:, inner_width:]).astype(
            jnp.bfloat16
        )
        product = jnp.dot(hidden, down_weight[local], preferred_element_type=jnp.float32)
        total = total + share[:, None] * product
    return lax.psum_scatter(total.astype(jnp.bfloat16), AXES, scatter_dimension=0, tiled=True)


def block_of(width, most):
    return max(b for b in range(LANES, most + 1, LANES) if width % b == 0)


def pick(table, z):
    value = jnp.int32(table[0])
    for k in range(1, len(table)):
        value = jnp.where(z == k, jnp.int32(table[k]), value)
    return value


def near_first(z, line):
    order = [z]
    for d in range(1, line):
        order += [j for j in (z - d, z + d) if 0 <= j < line]
    return order


def send_order(z, line):
    order = near_first(z, line)
    return order[1:2] + order[2:][::-1] + order[:1]


def kernel(
    line, experts, x_ref, wgu_hbm, wd_hbm, out_ref,
    tok, part, near, chain, wg, wd, acc, hid,
    x_sem, up_s, dn_s, y_s, tok_r, w_l, w_s, w_r, n_s, n_r, c_s, c_r,
):
    rows, width = out_ref.shape
    inner = wd.shape[1]
    e = lax.axis_index("ep")
    c = lax.axis_index("node")
    z, y = e // PAIR, e % PAIR
    other = 1 - y
    first, last = z == 0, z == line - 1
    has_dn, has_up = z > 0, z < line - 1
    to_up, to_dn = {"ep": e + PAIR}, {"ep": e - PAIR}
    to_y, to_core = {"ep": z * PAIR + other}, {"node": 1 - c}

    barrier = pltpu.get_barrier_semaphore()

    def greet(target):
        pl.semaphore_signal(barrier, inc=1, device_id=target, device_id_type=MESH)

    greet(to_core)
    greet(to_y)
    pl.when(has_up)(lambda: greet(to_up))
    pl.when(has_dn)(lambda: greet(to_dn))
    pl.semaphore_wait(barrier, 2 + jnp.where(has_up, 1, 0) + jnp.where(has_dn, 1, 0))

    def remote(src, dst, s, r, target):
        return pltpu.make_async_remote_copy(
            src_ref=src, dst_ref=dst, send_sem=s, recv_sem=r,
            device_id=target, device_id_type=MESH,
        )

    def tok_copy(j, sems, target, own=False):
        src = x_ref if own else tok.at[j, y]
        return remote(src, tok.at[j, y], sems.at[j], tok_r.at[j, y], target)

    def tok_arrived(j, row):
        remote(tok.at[j, row], tok.at[j, row], up_s.at[j], tok_r.at[j, row], to_y).wait_recv()

    def forward(d):
        own = d == 0

        def below():
            j = z - d
            if not own:
                tok_arrived(j, y)
            pl.when(has_up)(lambda: tok_copy(j, up_s, to_up, own).start())
            if own:
                pl.when(has_dn)(lambda: tok_copy(j, dn_s, to_dn, own).start())
            tok_copy(j, y_s, to_y, own).start()

        def above():
            j = z + d
            tok_arrived(j, y)
            pl.when(has_dn)(lambda: tok_copy(j, dn_s, to_dn).start())
            tok_copy(j, y_s, to_y).start()

        if own:
            below()
        else:
            pl.when(z >= d)(below)
            pl.when(z + d < line)(above)

    forward(0)
    own_copy = pltpu.make_async_copy(x_ref, tok.at[z, y], x_sem)
    own_copy.start()
    local = [
        pltpu.make_async_copy(wgu_hbm.at[0], wg.at[0], w_l.at[0]),
        pltpu.make_async_copy(wd_hbm.at[0], wd.at[0], w_l.at[1]),
    ]
    swapped = [
        remote(wgu_hbm.at[0], wg.at[1], w_s.at[0], w_r.at[0], to_core),
        remote(wd_hbm.at[0], wd.at[1], w_s.at[1], w_r.at[1], to_core),
    ]
    for copy in swapped + local:
        copy.start()

    mine = e * 2 + c
    names = (mine, e * 2 + 1 - c)
    k_block, n_block = block_of(width, 1792), block_of(width, 1024)

    def compute(p):
        j = pick([near_first(k, line)[p] for k in range(line)], z)
        tok_arrived(j, other)
        if p == 0:
            own_copy.wait()
            local[0].wait()
            swapped[0].wait_recv()
        acc[...] = jnp.zeros_like(acc)

        def up_step(k, carry):
            at = pl.ds(pl.multiple_of(k * k_block, k_block), k_block)
            block = tok[j, :, :, at].reshape(PAIR * rows, k_block)
            for s in range(2):
                acc[s] += jnp.dot(block, wg[s, at, :], preferred_element_type=jnp.float32)
            return carry

        lax.fori_loop(0, width // k_block, up_step, 0)
        for s in range(2):
            gate, up = acc[s, :, :inner], acc[s, :, inner:]
            hid[s] = (jax.nn.silu(gate) * up).astype(jnp.bfloat16)
        meta = tok[j, :, :, width:].astype(jnp.float32).reshape(PAIR * rows, -1)
        lane = lax.broadcasted_iota(jnp.int32, meta.shape, 1)
        shares = [
            jnp.sum(
                jnp.where((lane == name) | (lane == name + experts), meta, 0.0),
                axis=1, keepdims=True,
            )
            for name in names
        ]
        if p == 0:
            local[1].wait()
            swapped[1].wait_recv()

        def down_step(n, carry):
            at = pl.ds(pl.multiple_of(n * n_block, n_block), n_block)
            total = 0.0
            for s in range(2):
                total += shares[s] * jnp.dot(
                    hid[s], wd[s, :, at], preferred_element_type=jnp.float32
                )
            part[j, :, :, at] = total.astype(jnp.bfloat16).reshape(PAIR, rows, n_block)
            return carry

        lax.fori_loop(0, width // n_block, down_step, 0)

    piece = width // PIECES

    def near_copy(j, q):
        at = pl.ds(q * piece, piece)
        return remote(
            part.at[j, other, :, at], near.at[j, :, at], n_s.at[j, q], n_r.at[j, q], to_y
        )

    def send_near(p):
        j = pick([send_order(k, line)[p] for k in range(line)], z)
        for q in range(PIECES):
            near_copy(j, q).start()

    for d in range(1, line):
        forward(d)
        if d == line - 1:
            break
        compute(d - 1)
    compute(line - 2)
    send_near(0)
    compute(line - 1)
    for p in range(1, line):
        send_near(p)

    def chain_copy(j, slot, q, target):
        at = pl.ds(q * piece, piece)
        return remote(
            part.at[j, y, :, at], chain.at[slot, :, at], c_s.at[j, q], c_r.at[slot, q], target
        )

    def chain_arrived(slot, q):
        chain_copy(0, slot, q, to_y).wait_recv()

    def chain_up(j, d, q, start):
        copy = chain_copy(j, j, q, to_up)
        copy.start() if start else copy.wait_send()

    def chain_dn(j, d, q, start):
        copy = chain_copy(j, line if d == 1 else j, q, to_dn)
        copy.start() if start else copy.wait_send()

    def hop(j, q, came, push):
        at = pl.ds(q * piece, piece)
        near_copy(j, q).wait_recv()
        pl.when(came)(lambda: chain_arrived(j, q))
        total = part[j, y, :, at].astype(jnp.float32) + near[j, :, at].astype(jnp.float32)

        @pl.when(came)
        def _():
            part[j, y, :, at] = (total + chain[j, :, at].astype(jnp.float32)).astype(jnp.bfloat16)

        @pl.when(jnp.logical_not(came))
        def _():
            part[j, y, :, at] = total.astype(jnp.bfloat16)

        push()

    for d in range(line - 1, 0, -1):
        for q in range(PIECES):
            pl.when(z + d < line)(functools.partial(
                lambda d, q: hop(z + d, q, has_dn, lambda: chain_up(z + d, d, q, True)), d, q))
            pl.when(z >= d)(functools.partial(
                lambda d, q: hop(z - d, q, has_up, lambda: chain_dn(z - d, d, q, True)), d, q))

    for q in range(PIECES):
        at = pl.ds(q * piece, piece)
        near_copy(z, q).wait_recv()
        pl.when(has_dn)(lambda: chain_arrived(z, q))
        pl.when(has_up)(lambda: chain_arrived(line, q))
        total = part[z, y, :, at].astype(jnp.float32) + near[z, :, at].astype(jnp.float32)
        below = chain[z, :, at].astype(jnp.float32)
        above = chain[line, :, at].astype(jnp.float32)

        @pl.when(has_dn & has_up)
        def _():
            out_ref[:, at] = (total + below + above).astype(jnp.bfloat16)

        @pl.when(first)
        def _():
            out_ref[:, at] = (total + above).astype(jnp.bfloat16)

        @pl.when(last)
        def _():
            out_ref[:, at] = (total + below).astype(jnp.bfloat16)

    for copy in swapped:
        copy.wait_send()
    for d in range(line):
        own = d == 0

        def below(d=d, own=own):
            pl.when(has_up)(lambda: tok_copy(z - d, up_s, to_up, own).wait_send())
            if own:
                pl.when(has_dn)(lambda: tok_copy(z, dn_s, to_dn, own).wait_send())
            else:
                for q in range(PIECES):
                    chain_dn(z - d, d, q, False)
            tok_copy(z - d, y_s, to_y, own).wait_send()
            for q in range(PIECES):
                near_copy(z - d, q).wait_send()

        def above(d=d):
            pl.when(has_dn)(lambda: tok_copy(z + d, dn_s, to_dn).wait_send())
            tok_copy(z + d, y_s, to_y).wait_send()
            for q in range(PIECES):
                chain_up(z + d, d, q, False)
                near_copy(z + d, q).wait_send()

        if own:
            below()
        else:
            pl.when(z >= d)(below)
            pl.when(z + d < line)(above)


def on_grid(line, tokens, expert_ids, gate_weights, gate_up_weight, down_weight):
    experts = lax.axis_size("ep") * lax.axis_size("node")
    rows, width = tokens.shape
    inner = down_weight.shape[1]
    chosen = expert_ids[:, :, None] == jnp.arange(experts, dtype=jnp.int32)
    share = jnp.sum(jnp.where(chosen, gate_weights[:, :, None], 0.0), axis=1)
    high = lax.reduce_precision(share, 8, 7)
    tail = -2 * experts % LANES
    rest = jnp.pad(jnp.concatenate([high, share - high], axis=1), ((0, 0), (0, tail)))
    x = jnp.concatenate([tokens, rest.astype(jnp.bfloat16)], axis=1)
    dma, vmem, bf = pltpu.SemaphoreType.DMA, pltpu.VMEM, jnp.bfloat16
    return pl.pallas_call(
        functools.partial(kernel, line, experts),
        out_shape=jax.ShapeDtypeStruct((rows, width), bf),
        in_specs=[
            pl.BlockSpec(memory_space=pltpu.VMEM),
            pl.BlockSpec(memory_space=pl.ANY),
            pl.BlockSpec(memory_space=pl.ANY),
        ],
        out_specs=pl.BlockSpec(memory_space=pltpu.VMEM),
        scratch_shapes=[
            vmem((line, PAIR, rows, x.shape[1]), bf),
            vmem((line, PAIR, rows, width), bf),
            vmem((line, rows, width), bf),
            vmem((line + 1, rows, width), bf),
            vmem((2, width, 2 * inner), bf),
            vmem((2, inner, width), bf),
            vmem((2, PAIR * rows, 2 * inner), jnp.float32),
            vmem((2, PAIR * rows, inner), bf),
            dma(()), dma((line,)), dma((line,)), dma((line,)), dma((line, PAIR)),
            dma((2,)), dma((2,)), dma((2,)),
            dma((line, PIECES)), dma((line, PIECES)),
            dma((line, PIECES)), dma((line + 1, PIECES)),
        ],
        compiler_params=pltpu.CompilerParams(
            collective_id=0, has_side_effects=True, vmem_limit_bytes=VMEM_BYTES
        ),
    )(x, gate_up_weight, down_weight)


def on_device(tokens, expert_ids, gate_weights, gate_up_weight, down_weight):
    chips, cores = lax.axis_size("ep"), lax.axis_size("node")
    line = chips // PAIR
    rows, width = tokens.shape
    inner = down_weight.shape[1]
    planes = (5 * line + 2 * PAIR) * rows * width * 2 + 6 * inner * width * 2 * 1.1
    args = (tokens, expert_ids, gate_weights, gate_up_weight, down_weight)
    fits = planes < 0.9 * VMEM_BYTES and gate_up_weight.shape[0] == 1
    paired = cores == 2 and lax.axis_size("groups") * PAIR == 4
    if fits and paired and chips % PAIR == 0 and line > 1:
        return on_grid(line, *args)
    return spread_out(*args)


def solution(mesh):
    placed = (
        P(("groups", "ep", "node"), None),
        P(("groups", "ep", "node"), None),
        P(("groups", "ep", "node"), None),
        P(("ep", "node"), None, None),
        P(("ep", "node"), None, None),
    )
    return jax.shard_map(
        on_device,
        mesh=mesh,
        in_specs=placed,
        out_specs=P(("groups", "ep", "node"), None),
        check_vma=False,
    )
```

```python
import functools

import jax
import jax.numpy as jnp
from jax import lax
from jax.experimental import pallas as pl
from jax.experimental.pallas import tpu as pltpu
from jax.sharding import PartitionSpec as P

AXES = ("ep", "node")
PAIR = 2
PIECES = 2
SIDE = 7
LANES = 128
VMEM_BYTES = 60 * 1024 * 1024
MESH = pl.DeviceIdType.MESH


def spread_out(tokens, expert_ids, gate_weights, gate_up_weight, down_weight):
    local_count, inner_width = down_weight.shape[0], down_weight.shape[1]
    device = lax.axis_index("ep") * lax.axis_size("node") + lax.axis_index("node")
    all_tokens = lax.all_gather(tokens, AXES, axis=0, tiled=True)
    all_ids = lax.all_gather(expert_ids, AXES, axis=0, tiled=True)
    all_weights = lax.all_gather(gate_weights, AXES, axis=0, tiled=True)
    total = 0.0
    for local in range(local_count):
        expert = device * local_count + local
        share = jnp.sum(jnp.where(all_ids == expert, all_weights, 0.0), axis=1)
        gate_up = jnp.dot(all_tokens, gate_up_weight[local], preferred_element_type=jnp.float32)
        hidden = (jax.nn.silu(gate_up[:, :inner_width]) * gate_up[:, inner_width:]).astype(
            jnp.bfloat16
        )
        product = jnp.dot(hidden, down_weight[local], preferred_element_type=jnp.float32)
        total = total + share[:, None] * product
    return lax.psum_scatter(total.astype(jnp.bfloat16), AXES, scatter_dimension=0, tiled=True)


def block_of(width, most):
    return max(b for b in range(LANES, most + 1, LANES) if width % b == 0)


def pick(table, z):
    value = jnp.int32(table[0])
    for k in range(1, len(table)):
        value = jnp.where(z == k, jnp.int32(table[k]), value)
    return value


def near_first(z, line):
    order = [z]
    for d in range(1, line):
        order += [j for j in (z - d, z + d) if 0 <= j < line]
    return order


def send_order(z, line):
    order = near_first(z, line)
    return order[1:2] + order[2:][::-1] + order[:1]


def kernel(
    line, experts, x_ref, wgu_hbm, wd_hbm, out_ref,
    tok, part, near, chain, near_b, chain_b, wg, wd, acc, hid,
    x_sem, up_s, dn_s, y_s, tok_r, w_l, w_s, w_r, n_s, n_r, c_s, c_r,
    up_b, dn_b, y_b, tok_b, nb_s, nb_r, cb_s, cb_r,
):
    rows, width = out_ref.shape
    inner = wd.shape[1]
    main = width - near_b.shape[1]
    side = pl.ds(main, width - main)
    e = lax.axis_index("ep")
    c = lax.axis_index("node")
    z, y = e // PAIR, e % PAIR
    other = 1 - y
    first, last = z == 0, z == line - 1
    has_dn, has_up = z > 0, z < line - 1
    to_up, to_dn = {"ep": e + PAIR}, {"ep": e - PAIR}
    to_y, to_core = {"ep": z * PAIR + other}, {"node": 1 - c}

    barrier = pltpu.get_barrier_semaphore()

    def greet(target):
        pl.semaphore_signal(barrier, inc=1, device_id=target, device_id_type=MESH)

    greet(to_core)
    greet(to_y)
    pl.when(has_up)(lambda: greet(to_up))
    pl.when(has_dn)(lambda: greet(to_dn))
    pl.semaphore_wait(barrier, 2 + jnp.where(has_up, 1, 0) + jnp.where(has_dn, 1, 0))

    def remote(src, dst, s, r, target):
        return pltpu.make_async_remote_copy(
            src_ref=src, dst_ref=dst, send_sem=s, recv_sem=r,
            device_id=target, device_id_type=MESH,
        )

    def tok_copy(j, sems, target, own=False):
        at = pl.ds(0, main)
        src = x_ref.at[:, at] if own else tok.at[j, y, :, at]
        return remote(src, tok.at[j, y, :, at], sems.at[j], tok_r.at[j, y], target)

    def tok_arrived(j, row):
        ref = tok.at[j, row, :, pl.ds(0, main)]
        remote(ref, ref, up_s.at[j], tok_r.at[j, row], to_y).wait_recv()

    def side_copy(j, row, sem, target, own=False):
        at = pl.ds(main, x_ref.shape[1] - main)
        src = x_ref.at[:, at] if own else tok.at[j, row, :, at]
        return remote(src, tok.at[j, row, :, at], sem, tok_b.at[j, row], target)

    def side_up(j, row, own=False):
        return side_copy(j, row, up_b.at[j, row], to_up, own)

    def side_dn(j, row, own=False):
        return side_copy(j, row, dn_b.at[j, row], to_dn, own)

    def forward(d):
        own = d == 0

        def below():
            j = z - d
            if own:
                side_copy(j, y, y_b, to_y, own).start()
            else:
                tok_arrived(j, y)
            pl.when(has_up)(lambda: tok_copy(j, up_s, to_up, own).start())
            if own:
                pl.when(has_dn)(lambda: tok_copy(j, dn_s, to_dn, own).start())
            tok_copy(j, y_s, to_y, own).start()
            for row in (y, other):
                mine = own and row is y
                if not mine:
                    side_up(j, row).wait_recv()
                pl.when(has_up)(lambda: side_up(j, row, mine).start())
                if own:
                    pl.when(has_dn)(lambda: side_dn(j, row, mine).start())

        def above():
            j = z + d
            tok_arrived(j, y)
            pl.when(has_dn)(lambda: tok_copy(j, dn_s, to_dn).start())
            tok_copy(j, y_s, to_y).start()
            for row in (y, other):
                side_dn(j, row).wait_recv()
                pl.when(has_dn)(lambda: side_dn(j, row).start())

        if own:
            below()
        else:
            pl.when(z >= d)(below)
            pl.when(z + d < line)(above)

    own_copy = pltpu.make_async_copy(x_ref, tok.at[z, y], x_sem)
    own_copy.start()
    local = [
        pltpu.make_async_copy(wgu_hbm.at[0], wg.at[0], w_l.at[0]),
        pltpu.make_async_copy(wd_hbm.at[0], wd.at[0], w_l.at[1]),
    ]
    swapped = [
        remote(wgu_hbm.at[0], wg.at[1], w_s.at[0], w_r.at[0], to_core),
        remote(wd_hbm.at[0], wd.at[1], w_s.at[1], w_r.at[1], to_core),
    ]
    for copy in swapped + local:
        copy.start()

    forward(0)
    mine = e * 2 + c
    names = (mine, e * 2 + 1 - c)
    k_block, n_block = block_of(width, 1792), block_of(width, 1024)

    def compute(p):
        j = pick([near_first(k, line)[p] for k in range(line)], z)
        tok_arrived(j, other)
        if p == 0:
            own_copy.wait()
            local[0].wait()
            swapped[0].wait_recv()
        acc[...] = jnp.zeros_like(acc)

        def up_step(k, carry):
            at = pl.ds(pl.multiple_of(k * k_block, k_block), k_block)
            block = tok[j, :, :, at].reshape(PAIR * rows, k_block)
            for s in range(2):
                acc[s] += jnp.dot(block, wg[s, at, :], preferred_element_type=jnp.float32)
            return carry

        lax.fori_loop(0, width // k_block, up_step, 0)
        for s in range(2):
            gate, up = acc[s, :, :inner], acc[s, :, inner:]
            hid[s] = (jax.nn.silu(gate) * up).astype(jnp.bfloat16)
        meta = tok[j, :, :, width:].astype(jnp.float32).reshape(PAIR * rows, -1)
        lane = lax.broadcasted_iota(jnp.int32, meta.shape, 1)
        shares = [
            jnp.sum(
                jnp.where((lane == name) | (lane == name + experts), meta, 0.0),
                axis=1, keepdims=True,
            )
            for name in names
        ]
        if p == 0:
            local[1].wait()
            swapped[1].wait_recv()

        def down_step(n, carry):
            at = pl.ds(pl.multiple_of(n * n_block, n_block), n_block)
            total = 0.0
            for s in range(2):
                total += shares[s] * jnp.dot(
                    hid[s], wd[s, :, at], preferred_element_type=jnp.float32
                )
            part[j, :, :, at] = total.astype(jnp.bfloat16).reshape(PAIR, rows, n_block)
            return carry

        lax.fori_loop(0, width // n_block, down_step, 0)

    piece = main // PIECES

    def near_copy(j, q):
        at = pl.ds(q * piece, piece)
        return remote(
            part.at[j, other, :, at], near.at[j, :, at], n_s.at[j, q], n_r.at[j, q], to_y
        )

    def send_near(p):
        j = pick([send_order(k, line)[p] for k in range(line)], z)
        for q in range(PIECES):
            near_copy(j, q).start()

    for d in range(1, line):
        forward(d)
        if d == line - 1:
            break
        compute(d - 1)
    compute(line - 2)
    send_near(0)
    compute(line - 1)
    for p in range(1, line):
        send_near(p)

    def chain_copy(j, slot, q, target):
        at = pl.ds(q * piece, piece)
        return remote(
            part.at[j, y, :, at], chain.at[slot, :, at], c_s.at[j, q], c_r.at[slot, q], target
        )

    def chain_arrived(slot, q):
        chain_copy(0, slot, q, to_y).wait_recv()

    def chain_up(j, d, q, start):
        copy = chain_copy(j, j, q, to_up)
        copy.start() if start else copy.wait_send()

    def chain_dn(j, d, q, start):
        copy = chain_copy(j, line if d == 1 else j, q, to_dn)
        copy.start() if start else copy.wait_send()

    def hop(j, q, came, push):
        at = pl.ds(q * piece, piece)
        near_copy(j, q).wait_recv()
        pl.when(came)(lambda: chain_arrived(j, q))
        total = part[j, y, :, at].astype(jnp.float32) + near[j, :, at].astype(jnp.float32)

        @pl.when(came)
        def _():
            part[j, y, :, at] = (total + chain[j, :, at].astype(jnp.float32)).astype(jnp.bfloat16)

        @pl.when(jnp.logical_not(came))
        def _():
            part[j, y, :, at] = total.astype(jnp.bfloat16)

        push()

    def side_sum(j, row, d, came, upward, start):
        slot = line if d == 1 and not upward else j
        copy = remote(
            part.at[j, row, :, side], chain_b.at[slot, row], cb_s.at[j, row],
            cb_r.at[slot, row], to_up if upward else to_dn,
        )
        if not start:
            copy.wait_send()
            return

        @pl.when(came)
        def _():
            side_arrived(j, row)
            total = part[j, row, :, side].astype(jnp.float32)
            total += chain_b[j, row].astype(jnp.float32)
            part[j, row, :, side] = total.astype(jnp.bfloat16)

        copy.start()

    def side_arrived(slot, row):
        ref = chain_b.at[slot, row]
        remote(ref, ref, cb_s.at[0, row], cb_r.at[slot, row], to_y).wait_recv()

    def side_total(row):
        pl.when(has_dn)(lambda: side_arrived(z, row))
        pl.when(has_up)(lambda: side_arrived(line, row))
        below, above = chain_b[z, row].astype(jnp.float32), chain_b[line, row].astype(jnp.float32)
        total = part[z, row, :, side].astype(jnp.float32)
        return total + jnp.where(has_dn, below, 0.0) + jnp.where(has_up, above, 0.0)

    side_near = remote(part.at[z, other, :, side], near_b, nb_s, nb_r, to_y)
    for d in range(line - 1, 0, -1):
        for row in range(PAIR):
            pl.when(z + d < line)(functools.partial(
                lambda d, row: side_sum(z + d, row, d, has_dn, True, True), d, row))
            pl.when(z >= d)(functools.partial(
                lambda d, row: side_sum(z - d, row, d, has_up, False, True), d, row))
    part[z, other, :, side] = side_total(other).astype(jnp.bfloat16)
    side_near.start()
    side_total_own = side_total(y)

    for d in range(line - 1, 0, -1):
        for q in range(PIECES):
            pl.when(z + d < line)(functools.partial(
                lambda d, q: hop(z + d, q, has_dn, lambda: chain_up(z + d, d, q, True)), d, q))
            pl.when(z >= d)(functools.partial(
                lambda d, q: hop(z - d, q, has_up, lambda: chain_dn(z - d, d, q, True)), d, q))

    for q in range(PIECES):
        at = pl.ds(q * piece, piece)
        near_copy(z, q).wait_recv()
        pl.when(has_dn)(lambda: chain_arrived(z, q))
        pl.when(has_up)(lambda: chain_arrived(line, q))
        total = part[z, y, :, at].astype(jnp.float32) + near[z, :, at].astype(jnp.float32)
        below = chain[z, :, at].astype(jnp.float32)
        above = chain[line, :, at].astype(jnp.float32)

        @pl.when(has_dn & has_up)
        def _():
            out_ref[:, at] = (total + below + above).astype(jnp.bfloat16)

        @pl.when(first)
        def _():
            out_ref[:, at] = (total + above).astype(jnp.bfloat16)

        @pl.when(last)
        def _():
            out_ref[:, at] = (total + below).astype(jnp.bfloat16)

    side_near.wait_recv()
    out_ref[:, side] = (side_total_own + near_b[...].astype(jnp.float32)).astype(jnp.bfloat16)

    side_near.wait_send()
    side_copy(z, y, y_b, to_y, True).wait_send()
    for copy in swapped:
        copy.wait_send()
    for d in range(line):
        own = d == 0

        def below(d=d, own=own):
            pl.when(has_up)(lambda: tok_copy(z - d, up_s, to_up, own).wait_send())
            for row in range(PAIR):
                pl.when(has_up)(lambda row=row: side_up(z - d, row).wait_send())
                if own:
                    pl.when(has_dn)(lambda row=row: side_dn(z, row).wait_send())
                else:
                    side_sum(z - d, row, d, None, False, False)
            if own:
                pl.when(has_dn)(lambda: tok_copy(z, dn_s, to_dn, own).wait_send())
            else:
                for q in range(PIECES):
                    chain_dn(z - d, d, q, False)
            tok_copy(z - d, y_s, to_y, own).wait_send()
            for q in range(PIECES):
                near_copy(z - d, q).wait_send()

        def above(d=d):
            pl.when(has_dn)(lambda: tok_copy(z + d, dn_s, to_dn).wait_send())
            for row in range(PAIR):
                pl.when(has_dn)(lambda row=row: side_dn(z + d, row).wait_send())
                side_sum(z + d, row, d, None, True, False)
            tok_copy(z + d, y_s, to_y).wait_send()
            for q in range(PIECES):
                chain_up(z + d, d, q, False)
                near_copy(z + d, q).wait_send()

        if own:
            below()
        else:
            pl.when(z >= d)(below)
            pl.when(z + d < line)(above)


def on_grid(line, tokens, expert_ids, gate_weights, gate_up_weight, down_weight):
    experts = lax.axis_size("ep") * lax.axis_size("node")
    rows, width = tokens.shape
    inner = down_weight.shape[1]
    chosen = expert_ids[:, :, None] == jnp.arange(experts, dtype=jnp.int32)
    share = jnp.sum(jnp.where(chosen, gate_weights[:, :, None], 0.0), axis=1)
    high = lax.reduce_precision(share, 8, 7)
    tail = -2 * experts % LANES
    rest = jnp.pad(jnp.concatenate([high, share - high], axis=1), ((0, 0), (0, tail)))
    x = jnp.concatenate([tokens, rest.astype(jnp.bfloat16)], axis=1)
    step = LANES * PIECES
    side = width - (width - width // SIDE) // step * step
    dma, vmem, bf = pltpu.SemaphoreType.DMA, pltpu.VMEM, jnp.bfloat16
    return pl.pallas_call(
        functools.partial(kernel, line, experts),
        out_shape=jax.ShapeDtypeStruct((rows, width), bf),
        in_specs=[
            pl.BlockSpec(memory_space=pltpu.VMEM),
            pl.BlockSpec(memory_space=pl.ANY),
            pl.BlockSpec(memory_space=pl.ANY),
        ],
        out_specs=pl.BlockSpec(memory_space=pltpu.VMEM),
        scratch_shapes=[
            vmem((line, PAIR, rows, x.shape[1]), bf),
            vmem((line, PAIR, rows, width), bf),
            vmem((line, rows, width - side), bf),
            vmem((line + 1, rows, width - side), bf),
            vmem((rows, side), bf),
            vmem((line + 1, PAIR, rows, side), bf),
            vmem((2, width, 2 * inner), bf),
            vmem((2, inner, width), bf),
            vmem((2, PAIR * rows, 2 * inner), jnp.float32),
            vmem((2, PAIR * rows, inner), bf),
            dma(()), dma((line,)), dma((line,)), dma((line,)), dma((line, PAIR)),
            dma((2,)), dma((2,)), dma((2,)),
            dma((line, PIECES)), dma((line, PIECES)),
            dma((line, PIECES)), dma((line + 1, PIECES)),
            dma((line, PAIR)), dma((line, PAIR)), dma(()), dma((line, PAIR)),
            dma(()), dma(()), dma((line, PAIR)), dma((line + 1, PAIR)),
        ],
        compiler_params=pltpu.CompilerParams(
            collective_id=0, has_side_effects=True, vmem_limit_bytes=VMEM_BYTES
        ),
    )(x, gate_up_weight, down_weight)


def on_device(tokens, expert_ids, gate_weights, gate_up_weight, down_weight):
    chips, cores = lax.axis_size("ep"), lax.axis_size("node")
    line = chips // PAIR
    rows, width = tokens.shape
    inner = down_weight.shape[1]
    planes = (5 * line + 2 * PAIR) * rows * width * 2 + 6 * inner * width * 2 * 1.1
    args = (tokens, expert_ids, gate_weights, gate_up_weight, down_weight)
    fits = planes < 0.9 * VMEM_BYTES and gate_up_weight.shape[0] == 1
    paired = cores == 2 and lax.axis_size("groups") * PAIR == 4
    if fits and paired and chips % PAIR == 0 and line > 1:
        return on_grid(line, *args)
    return spread_out(*args)


def solution(mesh):
    placed = (
        P(("groups", "ep", "node"), None),
        P(("groups", "ep", "node"), None),
        P(("groups", "ep", "node"), None),
        P(("ep", "node"), None, None),
        P(("ep", "node"), None, None),
    )
    return jax.shard_map(
        on_device,
        mesh=mesh,
        in_specs=placed,
        out_specs=P(("groups", "ep", "node"), None),
        check_vma=False,
    )
```

```python
import functools

import jax
import jax.numpy as jnp
from jax import lax
from jax.experimental import pallas as pl
from jax.experimental.pallas import tpu as pltpu
from jax.sharding import PartitionSpec as P

AXES = ("ep", "node")
PAIR = 2
PIECES = 4
SIDE = 7
LANES = 128
VMEM_BYTES = 60 * 1024 * 1024
MESH = pl.DeviceIdType.MESH


def spread_out(tokens, expert_ids, gate_weights, gate_up_weight, down_weight):
    local_count, inner_width = down_weight.shape[0], down_weight.shape[1]
    device = lax.axis_index("ep") * lax.axis_size("node") + lax.axis_index("node")
    all_tokens = lax.all_gather(tokens, AXES, axis=0, tiled=True)
    all_ids = lax.all_gather(expert_ids, AXES, axis=0, tiled=True)
    all_weights = lax.all_gather(gate_weights, AXES, axis=0, tiled=True)
    total = 0.0
    for local in range(local_count):
        expert = device * local_count + local
        share = jnp.sum(jnp.where(all_ids == expert, all_weights, 0.0), axis=1)
        gate_up = jnp.dot(all_tokens, gate_up_weight[local], preferred_element_type=jnp.float32)
        hidden = (jax.nn.silu(gate_up[:, :inner_width]) * gate_up[:, inner_width:]).astype(
            jnp.bfloat16
        )
        product = jnp.dot(hidden, down_weight[local], preferred_element_type=jnp.float32)
        total = total + share[:, None] * product
    return lax.psum_scatter(total.astype(jnp.bfloat16), AXES, scatter_dimension=0, tiled=True)


def block_of(width, most):
    return max(b for b in range(LANES, most + 1, LANES) if width % b == 0)


def pick(table, z):
    value = jnp.int32(table[0])
    for k in range(1, len(table)):
        value = jnp.where(z == k, jnp.int32(table[k]), value)
    return value


def near_first(z, line):
    order = [z]
    for d in range(1, line):
        order += [j for j in (z - d, z + d) if 0 <= j < line]
    return order


def send_order(z, line):
    order = near_first(z, line)
    return order[1:] + order[:1]


def kernel(
    line, experts, x_ref, wgu_hbm, wd_hbm, out_ref,
    tok, part, near, chain, near_b, chain_b, wg, wd, acc, hid,
    x_sem, up_s, dn_s, y_s, tok_r, w_l, w_s, w_r, n_s, n_r, c_s, c_r,
    up_b, dn_b, y_b, tok_b, nb_s, nb_r, cb_s, cb_r,
):
    rows, width = out_ref.shape
    inner = wd.shape[1]
    main = width - near_b.shape[1]
    side = pl.ds(main, width - main)
    e = lax.axis_index("ep")
    c = lax.axis_index("node")
    z, y = e // PAIR, e % PAIR
    other = 1 - y
    first, last = z == 0, z == line - 1
    has_dn, has_up = z > 0, z < line - 1
    to_up, to_dn = {"ep": e + PAIR}, {"ep": e - PAIR}
    to_y, to_core = {"ep": z * PAIR + other}, {"node": 1 - c}

    barrier = pltpu.get_barrier_semaphore()

    def greet(target):
        pl.semaphore_signal(barrier, inc=1, device_id=target, device_id_type=MESH)

    greet(to_core)
    greet(to_y)
    pl.when(has_up)(lambda: greet(to_up))
    pl.when(has_dn)(lambda: greet(to_dn))
    pl.semaphore_wait(barrier, 2 + jnp.where(has_up, 1, 0) + jnp.where(has_dn, 1, 0))

    def remote(src, dst, s, r, target):
        return pltpu.make_async_remote_copy(
            src_ref=src, dst_ref=dst, send_sem=s, recv_sem=r,
            device_id=target, device_id_type=MESH,
        )

    def tok_copy(j, sems, target, own=False):
        at = pl.ds(0, main)
        src = x_ref.at[:, at] if own else tok.at[j, y, :, at]
        return remote(src, tok.at[j, y, :, at], sems.at[j], tok_r.at[j, y], target)

    def tok_arrived(j, row):
        ref = tok.at[j, row, :, pl.ds(0, main)]
        remote(ref, ref, up_s.at[j], tok_r.at[j, row], to_y).wait_recv()

    def side_copy(j, row, sem, target, own=False):
        at = pl.ds(main, x_ref.shape[1] - main)
        src = x_ref.at[:, at] if own else tok.at[j, row, :, at]
        return remote(src, tok.at[j, row, :, at], sem, tok_b.at[j, row], target)

    def side_up(j, row, own=False):
        return side_copy(j, row, up_b.at[j, row], to_up, own)

    def side_dn(j, row, own=False):
        return side_copy(j, row, dn_b.at[j, row], to_dn, own)

    def forward(d):
        own = d == 0

        def below():
            j = z - d
            if own:
                side_copy(j, y, y_b, to_y, own).start()
            else:
                tok_arrived(j, y)
            pl.when(has_up)(lambda: tok_copy(j, up_s, to_up, own).start())
            if own:
                pl.when(has_dn)(lambda: tok_copy(j, dn_s, to_dn, own).start())
            tok_copy(j, y_s, to_y, own).start()
            for row in (y, other):
                mine = own and row is y
                if not mine:
                    side_up(j, row).wait_recv()
                pl.when(has_up)(lambda: side_up(j, row, mine).start())
                if own:
                    pl.when(has_dn)(lambda: side_dn(j, row, mine).start())

        def above():
            j = z + d
            tok_arrived(j, y)
            pl.when(has_dn)(lambda: tok_copy(j, dn_s, to_dn).start())
            tok_copy(j, y_s, to_y).start()
            for row in (y, other):
                side_dn(j, row).wait_recv()
                pl.when(has_dn)(lambda: side_dn(j, row).start())

        if own:
            below()
        else:
            pl.when(z >= d)(below)
            pl.when(z + d < line)(above)

    own_copy = pltpu.make_async_copy(x_ref, tok.at[z, y], x_sem)
    own_copy.start()
    local = [
        pltpu.make_async_copy(wgu_hbm.at[0], wg.at[0], w_l.at[0]),
        pltpu.make_async_copy(wd_hbm.at[0], wd.at[0], w_l.at[1]),
    ]
    swapped = [
        remote(wgu_hbm.at[0], wg.at[1], w_s.at[0], w_r.at[0], to_core),
        remote(wd_hbm.at[0], wd.at[1], w_s.at[1], w_r.at[1], to_core),
    ]
    for copy in swapped + local:
        copy.start()

    forward(0)
    mine = e * 2 + c
    names = (mine, e * 2 + 1 - c)
    k_block, n_block = block_of(width, 1792), block_of(width, 1024)

    def compute(p):
        j = pick([near_first(k, line)[p] for k in range(line)], z)
        tok_arrived(j, other)
        if p == 0:
            own_copy.wait()
            local[0].wait()
            swapped[0].wait_recv()
        acc[...] = jnp.zeros_like(acc)

        def up_step(k, carry):
            at = pl.ds(pl.multiple_of(k * k_block, k_block), k_block)
            block = tok[j, :, :, at].reshape(PAIR * rows, k_block)
            for s in range(2):
                acc[s] += jnp.dot(block, wg[s, at, :], preferred_element_type=jnp.float32)
            return carry

        lax.fori_loop(0, width // k_block, up_step, 0)
        for s in range(2):
            gate, up = acc[s, :, :inner], acc[s, :, inner:]
            hid[s] = (jax.nn.silu(gate) * up).astype(jnp.bfloat16)
        meta = tok[j, :, :, width:].astype(jnp.float32).reshape(PAIR * rows, -1)
        lane = lax.broadcasted_iota(jnp.int32, meta.shape, 1)
        shares = [
            jnp.sum(
                jnp.where((lane == name) | (lane == name + experts), meta, 0.0),
                axis=1, keepdims=True,
            )
            for name in names
        ]
        if p == 0:
            local[1].wait()
            swapped[1].wait_recv()

        def down_step(n, carry):
            at = pl.ds(pl.multiple_of(n * n_block, n_block), n_block)
            total = 0.0
            for s in range(2):
                total += shares[s] * jnp.dot(
                    hid[s], wd[s, :, at], preferred_element_type=jnp.float32
                )
            part[j, :, :, at] = total.astype(jnp.bfloat16).reshape(PAIR, rows, n_block)
            return carry

        lax.fori_loop(0, width // n_block, down_step, 0)

    piece = main // PIECES

    def near_copy(j, q):
        at = pl.ds(q * piece, piece)
        return remote(
            part.at[j, other, :, at], near.at[j, :, at], n_s.at[j, q], n_r.at[j, q], to_y
        )

    def send_near(p):
        j = pick([send_order(k, line)[p] for k in range(line)], z)
        for q in range(PIECES):
            near_copy(j, q).start()

    for d in range(1, line):
        forward(d)
        if d == line - 1:
            break
        compute(d - 1)
    compute(line - 2)
    for p in range(line - 2):
        send_near(p)
    compute(line - 1)
    for p in range(line - 2, line):
        send_near(p)

    def chain_copy(j, slot, q, target):
        at = pl.ds(q * piece, piece)
        return remote(
            part.at[j, y, :, at], chain.at[slot, :, at], c_s.at[j, q], c_r.at[slot, q], target
        )

    def chain_arrived(slot, q):
        chain_copy(0, slot, q, to_y).wait_recv()

    def chain_up(j, d, q, start):
        copy = chain_copy(j, j, q, to_up)
        copy.start() if start else copy.wait_send()

    def chain_dn(j, d, q, start):
        copy = chain_copy(j, line if d == 1 else j, q, to_dn)
        copy.start() if start else copy.wait_send()

    def hop(j, q, came, push):
        at = pl.ds(q * piece, piece)
        near_copy(j, q).wait_recv()
        pl.when(came)(lambda: chain_arrived(j, q))
        total = part[j, y, :, at].astype(jnp.float32) + near[j, :, at].astype(jnp.float32)

        @pl.when(came)
        def _():
            part[j, y, :, at] = (total + chain[j, :, at].astype(jnp.float32)).astype(jnp.bfloat16)

        @pl.when(jnp.logical_not(came))
        def _():
            part[j, y, :, at] = total.astype(jnp.bfloat16)

        push()

    def side_sum(j, row, d, came, upward, start):
        slot = line if d == 1 and not upward else j
        copy = remote(
            part.at[j, row, :, side], chain_b.at[slot, row], cb_s.at[j, row],
            cb_r.at[slot, row], to_up if upward else to_dn,
        )
        if not start:
            copy.wait_send()
            return

        @pl.when(came)
        def _():
            side_arrived(j, row)
            total = part[j, row, :, side].astype(jnp.float32)
            total += chain_b[j, row].astype(jnp.float32)
            part[j, row, :, side] = total.astype(jnp.bfloat16)

        copy.start()

    def side_arrived(slot, row):
        ref = chain_b.at[slot, row]
        remote(ref, ref, cb_s.at[0, row], cb_r.at[slot, row], to_y).wait_recv()

    def side_total(row):
        pl.when(has_dn)(lambda: side_arrived(z, row))
        pl.when(has_up)(lambda: side_arrived(line, row))
        below, above = chain_b[z, row].astype(jnp.float32), chain_b[line, row].astype(jnp.float32)
        total = part[z, row, :, side].astype(jnp.float32)
        return total + jnp.where(has_dn, below, 0.0) + jnp.where(has_up, above, 0.0)

    side_near = remote(part.at[z, other, :, side], near_b, nb_s, nb_r, to_y)
    for d in range(line - 1, 0, -1):
        for row in range(PAIR):
            pl.when(z + d < line)(functools.partial(
                lambda d, row: side_sum(z + d, row, d, has_dn, True, True), d, row))
            pl.when(z >= d)(functools.partial(
                lambda d, row: side_sum(z - d, row, d, has_up, False, True), d, row))
    part[z, other, :, side] = side_total(other).astype(jnp.bfloat16)
    side_near.start()
    side_total_own = side_total(y)

    for d in range(line - 1, 0, -1):
        for q in range(PIECES):
            pl.when(z + d < line)(functools.partial(
                lambda d, q: hop(z + d, q, has_dn, lambda: chain_up(z + d, d, q, True)), d, q))
            pl.when(z >= d)(functools.partial(
                lambda d, q: hop(z - d, q, has_up, lambda: chain_dn(z - d, d, q, True)), d, q))

    for q in range(PIECES):
        at = pl.ds(q * piece, piece)
        near_copy(z, q).wait_recv()
        pl.when(has_dn)(lambda: chain_arrived(z, q))
        pl.when(has_up)(lambda: chain_arrived(line, q))
        total = part[z, y, :, at].astype(jnp.float32) + near[z, :, at].astype(jnp.float32)
        below = chain[z, :, at].astype(jnp.float32)
        above = chain[line, :, at].astype(jnp.float32)

        @pl.when(has_dn & has_up)
        def _():
            out_ref[:, at] = (total + below + above).astype(jnp.bfloat16)

        @pl.when(first)
        def _():
            out_ref[:, at] = (total + above).astype(jnp.bfloat16)

        @pl.when(last)
        def _():
            out_ref[:, at] = (total + below).astype(jnp.bfloat16)

    side_near.wait_recv()
    out_ref[:, side] = (side_total_own + near_b[...].astype(jnp.float32)).astype(jnp.bfloat16)

    side_near.wait_send()
    side_copy(z, y, y_b, to_y, True).wait_send()
    for copy in swapped:
        copy.wait_send()
    for d in range(line):
        own = d == 0

        def below(d=d, own=own):
            pl.when(has_up)(lambda: tok_copy(z - d, up_s, to_up, own).wait_send())
            for row in range(PAIR):
                pl.when(has_up)(lambda row=row: side_up(z - d, row).wait_send())
                if own:
                    pl.when(has_dn)(lambda row=row: side_dn(z, row).wait_send())
                else:
                    side_sum(z - d, row, d, None, False, False)
            if own:
                pl.when(has_dn)(lambda: tok_copy(z, dn_s, to_dn, own).wait_send())
            else:
                for q in range(PIECES):
                    chain_dn(z - d, d, q, False)
            tok_copy(z - d, y_s, to_y, own).wait_send()
            for q in range(PIECES):
                near_copy(z - d, q).wait_send()

        def above(d=d):
            pl.when(has_dn)(lambda: tok_copy(z + d, dn_s, to_dn).wait_send())
            for row in range(PAIR):
                pl.when(has_dn)(lambda row=row: side_dn(z + d, row).wait_send())
                side_sum(z + d, row, d, None, True, False)
            tok_copy(z + d, y_s, to_y).wait_send()
            for q in range(PIECES):
                chain_up(z + d, d, q, False)
                near_copy(z + d, q).wait_send()

        if own:
            below()
        else:
            pl.when(z >= d)(below)
            pl.when(z + d < line)(above)


def on_grid(line, tokens, expert_ids, gate_weights, gate_up_weight, down_weight):
    experts = lax.axis_size("ep") * lax.axis_size("node")
    rows, width = tokens.shape
    inner = down_weight.shape[1]
    chosen = expert_ids[:, :, None] == jnp.arange(experts, dtype=jnp.int32)
    share = jnp.sum(jnp.where(chosen, gate_weights[:, :, None], 0.0), axis=1)
    high = lax.reduce_precision(share, 8, 7)
    tail = -2 * experts % LANES
    rest = jnp.pad(jnp.concatenate([high, share - high], axis=1), ((0, 0), (0, tail)))
    x = jnp.concatenate([tokens, rest.astype(jnp.bfloat16)], axis=1)
    step = LANES * PIECES
    side = width - (width - width // SIDE) // step * step
    dma, vmem, bf = pltpu.SemaphoreType.DMA, pltpu.VMEM, jnp.bfloat16
    return pl.pallas_call(
        functools.partial(kernel, line, experts),
        out_shape=jax.ShapeDtypeStruct((rows, width), bf),
        in_specs=[
            pl.BlockSpec(memory_space=pltpu.VMEM),
            pl.BlockSpec(memory_space=pl.ANY),
            pl.BlockSpec(memory_space=pl.ANY),
        ],
        out_specs=pl.BlockSpec(memory_space=pltpu.VMEM),
        scratch_shapes=[
            vmem((line, PAIR, rows, x.shape[1]), bf),
            vmem((line, PAIR, rows, width), bf),
            vmem((line, rows, width - side), bf),
            vmem((line + 1, rows, width - side), bf),
            vmem((rows, side), bf),
            vmem((line + 1, PAIR, rows, side), bf),
            vmem((2, width, 2 * inner), bf),
            vmem((2, inner, width), bf),
            vmem((2, PAIR * rows, 2 * inner), jnp.float32),
            vmem((2, PAIR * rows, inner), bf),
            dma(()), dma((line,)), dma((line,)), dma((line,)), dma((line, PAIR)),
            dma((2,)), dma((2,)), dma((2,)),
            dma((line, PIECES)), dma((line, PIECES)),
            dma((line, PIECES)), dma((line + 1, PIECES)),
            dma((line, PAIR)), dma((line, PAIR)), dma(()), dma((line, PAIR)),
            dma(()), dma(()), dma((line, PAIR)), dma((line + 1, PAIR)),
        ],
        compiler_params=pltpu.CompilerParams(
            collective_id=0, has_side_effects=True, vmem_limit_bytes=VMEM_BYTES
        ),
    )(x, gate_up_weight, down_weight)


def on_device(tokens, expert_ids, gate_weights, gate_up_weight, down_weight):
    chips, cores = lax.axis_size("ep"), lax.axis_size("node")
    line = chips // PAIR
    rows, width = tokens.shape
    inner = down_weight.shape[1]
    planes = (5 * line + 2 * PAIR) * rows * width * 2 + 6 * inner * width * 2 * 1.1
    args = (tokens, expert_ids, gate_weights, gate_up_weight, down_weight)
    fits = planes < 0.9 * VMEM_BYTES and gate_up_weight.shape[0] == 1
    paired = cores == 2 and lax.axis_size("groups") * PAIR == 4
    if fits and paired and chips % PAIR == 0 and line > 1:
        return on_grid(line, *args)
    return spread_out(*args)


def solution(mesh):
    placed = (
        P(("groups", "ep", "node"), None),
        P(("groups", "ep", "node"), None),
        P(("groups", "ep", "node"), None),
        P(("ep", "node"), None, None),
        P(("ep", "node"), None, None),
    )
    return jax.shard_map(
        on_device,
        mesh=mesh,
        in_specs=placed,
        out_specs=P(("groups", "ep", "node"), None),
        check_vma=False,
    )
```
